256 devices in a mesh: gx: 8 (over x, core), gy: 8 (over z), gz: 4 (over y).
Axes of the slice: x: 4, y: 4, z: 8, core: 2. Of those that a mesh axis runs over, the one named last changes fastest.
Arguments:
- particle_mass: float32 [8388608], P(('gx', 'gy', 'gz')), may hold values from 0.5 to 2
- particle_velocity: float32 [3, 8388608], P(None, ('gx', 'gy', 'gz')), may hold values from -6 to 6
- particle_affine: float32 [9, 8388608], P(None, ('gx', 'gy', 'gz')), may hold values from -6 to 6
- particle_cell: int32 [3, 8388608], P(None, ('gx', 'gy', 'gz')), may hold values from 0 to 13
- particle_fraction: int32 [3, 8388608], P(None, ('gx', 'gy', 'gz')), may hold values from 0 to 1023
- block_owner: int32 [16384, 1], P(('gx', 'gy', 'gz')), may hold values from 0 to 31; in each aligned block of 64 rows (0 to 63, 64 to 127, ...) at most 4 rows name the same one
- block_slot: int32 [16384], P(('gx', 'gy', 'gz')), may hold values from 0 to 15
- block_count: int32 [16384], P(('gx', 'gy', 'gz')), may hold values from 128 to 512
- cell_drag: float32 [4096, 4096], P(('gx', 'gy', 'gz')), may hold values from 0.5 to 2
Outputs:
- grid_velocity: float32 [4096, 3, 4096], P(('gx', 'gy', 'gz'))
- new_velocity: float32 [3, 8388608], P(None, ('gx', 'gy', 'gz'))
- new_affine: float32 [9, 8388608], P(None, ('gx', 'gy', 'gz'))
The draws below stay inside these ranges and needn't reach their ends.
Inputs may be any that keep to these rules, and one draw needn't show every extreme that they name: `block_owner`: owner index counted over the devices with the particle device's own gx index, in gy+gz order; among the rows of one device, no owner is named more than 4 times. `block_count`: slots at or beyond the count are absent. `particle_cell`: A particle's three stencil nodes lie inside its grid block.
All inputs are finite; a program needn't handle non-finite values.
Results may differ from the reference program's by a relative error of at most 0.0085.
Values may be sent and summed in bfloat16 or wider, within the bound.
A program may use at most 128 MiB of HBM per device.

```python
import math
import jax
import jax.numpy as jnp
import numpy as np
from jax import lax

EDGE = 16
PB = 512
QUANT = 1024
BLK_DEV = 64
GROUP = 32
CAP = 4
TILES_DEV = 16
BLOCKS = 16384
PARTICLES = 8388608
TILES = 4096
CELLS = 4096
N_GY = 8
N_GZ = 4


def place_ends(entries, key, smallest, high):
    longest = entries.shape.index(max(entries.shape))
    spots = []
    for shift in (0, 1):
        where = [jax.random.randint(jax.random.fold_in(key, axis), (), 0, length) for axis, length in enumerate(entries.shape)]
        where[longest] = (where[longest] + shift) % entries.shape[longest]
        spots.append(tuple(where))
    return entries.at[spots[0]].set(smallest).at[spots[1]].set(high)


def block_levels(own_key, dims, shards, low, largest):
    def one(axis_at, blocks):
        heights = jax.random.uniform(jax.random.fold_in(jax.random.fold_in(own_key, 6), axis_at), (blocks,), jnp.float32, low / len(shards), largest / len(shards))
        return jnp.repeat(jnp.exp(heights), dims[axis_at] // blocks).reshape((-1,) + (1,) * (len(dims) - axis_at - 1))

    loudness = one(*shards[0])
    for cut in shards[1:]:
        loudness = loudness * one(*cut)
    return loudness


def shared_out(stream_key, own, number, rows, amount, top, most, slope):
    order = jax.random.permutation(stream_key, amount)
    packed, common = load_shares(amount, rows * top, most, slope, True), load_shares(amount, rows * top, most, slope, False)
    places = jnp.arange(amount)

    def named(lengths, rotation):
        used = int((lengths > 0).sum())
        fixed = max(1, used // 4)
        shifted = fixed + (places - fixed + rotation * (used - fixed)) % max(1, amount - fixed)
        return jnp.zeros((amount,), jnp.int32).at[order[jnp.where(places < fixed, places, shifted)]].set(jnp.asarray(lengths, jnp.int32))

    lengths = jnp.where(number % 4 == 0, named(packed, number // 4), named(common, number - number // 4 - 1))
    mixed = jax.random.permutation(jax.random.fold_in(own, 3), amount)
    giver, receiver = mixed[0:amount // 2 * 2:2], mixed[1:amount // 2 * 2:2]
    margin = jnp.minimum(lengths[giver] - 1, most - lengths[receiver]) // 2
    margin = jnp.where((giver == order[0]) | (receiver == order[0]) | (lengths[receiver] == 0), 0, jnp.maximum(margin, 0))
    shifted = jax.random.randint(jax.random.fold_in(own, 4), (amount // 2,), 0, 1 << 20) % (margin + 1)
    lengths = lengths.at[giver].add(-shifted).at[receiver].add(shifted)
    labels = jnp.searchsorted(jnp.cumsum(lengths), jnp.arange(rows * top), side="right").astype(jnp.int32)
    table = labels.reshape(top, rows).T
    table = table[jax.random.permutation(jax.random.fold_in(own, 1), rows)]
    rotation = jax.random.randint(jax.random.fold_in(own, 2), (rows, 1), 0, top)
    return jnp.take_along_axis(table, (jnp.arange(top)[None, :] + rotation) % top, axis=1)


def load_shares(amount, total, bound, slope, full):
    loads = [(1 << 20) // math.isqrt(standing ** slope) + 1 for standing in range(1, amount + 1)]
    largest = bound if full else min(bound, max(-(-total // amount), total * loads[0] // sum(loads)))
    least = 1 if total - largest >= amount - 1 else 0
    holding, rest = [largest] + [least] * (amount - 1), total - largest - least * (amount - 1)
    while rest > 0:
        free = [i for i in range(1, amount) if holding[i] < largest] or [i for i in range(1, amount) if holding[i] < bound]
        whole, budget = sum([loads[i] for i in free]), rest
        for i in free:
            more = min(bound - holding[i], max(1, budget * loads[i] // whole), rest)
            holding[i] = holding[i] + more
            rest = rest - more
    return np.array(holding)


def gaussian(stream_key, extent, deviation, reach, pieces=(), kind=jnp.bfloat16):
    result = deviation * jax.random.normal(stream_key, extent, jnp.float32)
    if pieces:
        result = result * block_levels(stream_key, extent, pieces, -0.22, 0.18)
    return jnp.clip(result, -reach, reach).astype(kind)


def setup_inputs(seed: int = 0) -> dict:
    keys = jax.random.split(jax.random.key(seed), 10)
    particle_mass = jnp.clip(jnp.exp(math.log(2.0) - 1.3862944 * jax.random.uniform(keys[0], (PARTICLES,), jnp.float32) ** block_levels(keys[0], (PARTICLES,), ((0, 256),), -0.2, 0.2)), 0.5, 2.0)
    particle_velocity = gaussian(keys[1], (3, PARTICLES), 1.0, 6.0, ((1, 256),), jnp.float32)
    particle_affine = gaussian(keys[2], (9, PARTICLES), 1.0, 6.0, ((1, 256),), jnp.float32)
    particle_cell = place_ends(jax.random.randint(keys[3], (3, PARTICLES), 0, EDGE - 2), jax.random.fold_in(keys[3], 1), 0, (EDGE - 2) - 1).astype(jnp.int32)
    particle_fraction = place_ends(jax.random.randint(keys[4], (3, PARTICLES), 0, QUANT), jax.random.fold_in(keys[4], 1), 0, QUANT - 1).astype(jnp.int32)
    block_owner_keys = jax.random.split(jax.random.fold_in(keys[5], 1), BLOCKS // BLK_DEV)
    block_owner_turns = jax.random.permutation(jax.random.fold_in(keys[5], 3), BLOCKS // BLK_DEV)
    block_owner = jax.vmap(lambda own, number: shared_out(jax.random.fold_in(keys[5], 2), own, number, BLK_DEV, GROUP, 1, CAP, 2))(block_owner_keys, block_owner_turns).reshape((BLOCKS, 1))
    block_slot = place_ends(jax.random.randint(keys[6], (BLOCKS,), 0, TILES_DEV), jax.random.fold_in(keys[6], 1), 0, TILES_DEV - 1).astype(jnp.int32)
    block_count = place_ends(jax.random.randint(keys[7], (BLOCKS,), PB // 4, PB + 1), jax.random.fold_in(keys[7], 1), PB // 4, PB).astype(jnp.int32)
    cell_drag = jnp.clip(jnp.exp(math.log(2.0) - 1.3862944 * jax.random.uniform(keys[8], (TILES, CELLS), jnp.float32) ** block_levels(keys[8], (TILES, CELLS), ((0, 256),), -0.2, 0.2)), 0.5, 2.0)
    return dict(particle_mass=particle_mass, particle_velocity=particle_velocity, particle_affine=particle_affine, particle_cell=particle_cell, particle_fraction=particle_fraction, block_owner=block_owner, block_slot=block_slot, block_count=block_count, cell_drag=cell_drag)


def spline(offset):
    magnitude = jnp.abs(offset)
    inner_part = 0.75 - magnitude * magnitude
    outer_part = 0.5 * (1.5 - magnitude) * (1.5 - magnitude)
    return jnp.where(magnitude < 0.5, inner_part, jnp.where(magnitude < 1.5, outer_part, 0.0))


def particle_table(particle_mass, particle_velocity, particle_affine, particle_cell, particle_fraction, block_count):
    blocks = block_count.shape[0]
    batch_shape = (blocks, particle_mass.shape[0] // blocks)
    places = jnp.arange(batch_shape[1], dtype=jnp.int32)
    present = places[None, :] < block_count[:, None]
    live_mass = jnp.where(present, particle_mass.reshape(batch_shape), 0.0)
    position = particle_cell.astype(jnp.float32) + 0.5 + (particle_fraction.astype(jnp.float32) + 0.5) / QUANT
    return jnp.concatenate([live_mass[None], particle_velocity.reshape((3,) + batch_shape), particle_affine.reshape((9,) + batch_shape), position.reshape((3,) + batch_shape)], axis=0)


def stencil(particle_data):
    node_coords = jnp.arange(EDGE, dtype=jnp.float32)
    offset = node_coords[None, :, None, None] - particle_data[13:16][:, None]
    weights = spline(offset)
    return weights, weights * offset


def planes(weights, slopes):
    def outer(first_factor, second_factor):
        product_table = first_factor[:, None] * second_factor[None, :]
        return product_table.reshape((EDGE * EDGE,) + product_table.shape[2:]).astype(jnp.bfloat16)
    return outer(weights[1], weights[2]), outer(slopes[1], weights[2]), outer(weights[1], slopes[2])


def deposit(particle_data):
    batch_shape = particle_data.shape[1:]
    weights, slopes = stencil(particle_data)
    plane_zero, plane_one, plane_two = planes(weights, slopes)
    live_mass = particle_data[0]
    along_x = weights[0]
    slope_x = slopes[0]
    affine = particle_data[4:13].reshape((3, 3) + batch_shape)
    mass_lead = (live_mass[None] * along_x)[None]
    momentum_lead = live_mass[None, None] * (particle_data[1:4][:, None] * along_x[None] + affine[:, 0][:, None] * slope_x[None])
    lead_zero = jnp.concatenate([mass_lead, momentum_lead], axis=0).astype(jnp.bfloat16)
    lead_one = (live_mass[None, None] * affine[:, 1][:, None] * along_x[None]).astype(jnp.bfloat16)
    lead_two = (live_mass[None, None] * affine[:, 2][:, None] * along_x[None]).astype(jnp.bfloat16)

    def contract(lead, plane):
        flattened = lead.reshape((-1,) + batch_shape).astype(jnp.float32)
        return jnp.einsum("anp,bnp->nab", flattened, plane.astype(jnp.float32), precision=lax.Precision.HIGHEST)

    count_blocks = batch_shape[0]
    dep_zero = contract(lead_zero, plane_zero).reshape(count_blocks, 4, -1)
    dep_one = contract(lead_one, plane_one).reshape(count_blocks, 3, -1)
    dep_two = contract(lead_two, plane_two).reshape(count_blocks, 3, -1)
    return jnp.concatenate([dep_zero[:, :1], dep_zero[:, 1:] + dep_one + dep_two], axis=1)


def interpolate(particle_data, grid_rows):
    batch_shape = particle_data.shape[1:]
    weights, slopes = stencil(particle_data)
    plane_zero, plane_one, plane_two = planes(weights, slopes)
    along_x = weights[0]
    slope_x = slopes[0]
    flattened = grid_rows.reshape(batch_shape[0], 3 * EDGE, EDGE * EDGE).astype(jnp.float32)

    def contract(plane):
        moment = jnp.einsum("nab,bnp->anp", flattened, plane.astype(jnp.float32), precision=lax.Precision.HIGHEST)
        return moment.reshape((3, EDGE) + batch_shape)

    moment_zero = contract(plane_zero)
    moment_one = contract(plane_one)
    moment_two = contract(plane_two)
    velocity_out = jnp.sum(along_x[None] * moment_zero, axis=1)
    column_zero = 4.0 * jnp.sum(slope_x[None] * moment_zero, axis=1)
    column_one = 4.0 * jnp.sum(along_x[None] * moment_one, axis=1)
    column_two = 4.0 * jnp.sum(along_x[None] * moment_two, axis=1)
    affine_out = jnp.stack([column_zero, column_one, column_two], axis=1).reshape((9,) + batch_shape)
    present = (particle_data[0] > 0.0).astype(jnp.float32)
    return jnp.concatenate([velocity_out, affine_out], axis=0) * present[None]


def reference(particle_mass, particle_velocity, particle_affine, particle_cell, particle_fraction, block_owner, block_slot, block_count, cell_drag):
    group_size = N_GY * N_GZ
    particle_data = particle_table(particle_mass, particle_velocity, particle_affine, particle_cell, particle_fraction, block_count)
    blocks = block_count.shape[0]
    device = jnp.arange(blocks, dtype=jnp.int32) // BLK_DEV
    tile_ids = (((device // group_size) * group_size + block_owner[:, 0]) * TILES_DEV + block_slot).astype(jnp.int32)

    def accumulate(grid_sums, block_index):
        portion = lax.dynamic_slice_in_dim(particle_data, block_index, 1, 1)
        return grid_sums.at[tile_ids[block_index]].add(deposit(portion)[0]), None

    initial = jnp.zeros((cell_drag.shape[0], 4, cell_drag.shape[1]), jnp.float32)
    grid_sums = lax.scan(accumulate, initial, jnp.arange(blocks, dtype=jnp.int32))[0]
    grid_velocity = grid_sums[:, 1:] / (grid_sums[:, :1] + cell_drag[:, None, :])
    rounded = grid_velocity.astype(jnp.bfloat16)

    def sample(block_index):
        portion = lax.dynamic_slice_in_dim(particle_data, block_index, 1, 1)
        cell_rows = lax.dynamic_index_in_dim(rounded, tile_ids[block_index], 0, keepdims=True)
        return interpolate(portion, cell_rows)[:, 0]

    finished = lax.map(sample, jnp.arange(blocks, dtype=jnp.int32))
    finished = jnp.transpose(finished, (1, 0, 2)).reshape(12, -1)
    return grid_velocity, finished[:3], finished[3:]
```

```python
import functools

import jax
import jax.numpy as jnp
from jax import lax
from jax.experimental import pallas as pl
from jax.experimental.pallas import tpu as pltpu
from jax.sharding import PartitionSpec as P

EDGE = 16
QUANT = 1024
PLANE = EDGE * EDGE
STEP_BLOCKS = 8


def stencil(cell_ref, fraction_ref, axis, columns):
    cell = cell_ref[axis : axis + 1, columns].astype(jnp.float32)
    fraction = fraction_ref[axis : axis + 1, columns].astype(jnp.float32)
    position = cell + 0.5 + (fraction + 0.5) / QUANT
    node = lax.broadcasted_iota(jnp.int32, (EDGE, position.shape[1]), 0).astype(jnp.float32)
    offset = node - position
    magnitude = jnp.abs(offset)
    inner = 0.75 - magnitude * magnitude
    reach = jnp.maximum(1.5 - magnitude, 0.0)
    weight = jnp.where(magnitude < 0.5, inner, 0.5 * reach * reach)
    return weight, weight * offset


def fill_planes(cell_ref, fraction_ref, columns, rows_ref, plane_ref):
    width = rows_ref.shape[1]
    weight_y, slope_y = stencil(cell_ref, fraction_ref, 1, columns)
    weight_z, slope_z = stencil(cell_ref, fraction_ref, 2, columns)
    rows_ref[0:EDGE, :] = weight_y
    rows_ref[EDGE : 2 * EDGE, :] = slope_y
    for y in range(EDGE):
        rows = slice(y * EDGE, (y + 1) * EDGE)
        along = rows_ref[y : y + 1, :]
        tilt = rows_ref[EDGE + y : EDGE + y + 1, :]
        plane_ref[rows, 0:width] = (along * weight_z).astype(jnp.bfloat16)
        plane_ref[rows, width : 2 * width] = (tilt * weight_z).astype(jnp.bfloat16)
        plane_ref[rows, 2 * width : 3 * width] = (along * slope_z).astype(jnp.bfloat16)


def deposit_kernel(
    owner_ref,
    slot_ref,
    count_ref,
    mass_ref,
    velocity_ref,
    affine_ref,
    cell_ref,
    fraction_ref,
    deposits_ref,
    place_ref,
    tiles_ref,
    used_ref,
    rows_ref,
    plane_ref,
    lead_ref,
    *,
    capacity,
    width,
):
    step = pl.program_id(0)
    groups = used_ref.shape[0]
    blocks = owner_ref.shape[0]

    @pl.when(step == 0)
    def _():
        deposits_ref[...] = jnp.zeros_like(deposits_ref)
        lead_ref[...] = jnp.zeros_like(lead_ref)

        @pl.loop(0, groups)
        def _(group):
            used_ref[group] = 0

        @pl.loop(0, groups * capacity)
        def _(slot):
            tiles_ref[slot] = -1

        @pl.loop(0, blocks)
        def _(block):
            owner = owner_ref[block]
            rank = used_ref[owner]
            used_ref[owner] = rank + 1
            place = owner * capacity + rank
            place_ref[block] = place
            tiles_ref[place] = slot_ref[block]

    def one_block(local, half):
        block = step * STEP_BLOCKS + local
        columns = pl.ds(pl.multiple_of(local * width, width), width)
        rows_half, plane_half, lead_half = rows_ref.at[half], plane_ref.at[half], lead_ref.at[half]
        fill_planes(cell_ref, fraction_ref, columns, rows_half, plane_half)
        weight, slope = stencil(cell_ref, fraction_ref, 0, columns)
        lane = lax.broadcasted_iota(jnp.int32, (1, width), 1)
        mass = jnp.where(lane < count_ref[block], mass_ref[0:1, columns], 0.0)
        lead_half[0:EDGE, 0:width] = (mass * weight).astype(jnp.bfloat16)
        for d in range(3):
            rows = slice((d + 1) * EDGE, (d + 2) * EDGE)
            velocity = velocity_ref[d : d + 1, columns]
            first = affine_ref[3 * d : 3 * d + 1, columns]
            second = mass * affine_ref[3 * d + 1 : 3 * d + 2, columns]
            third = mass * affine_ref[3 * d + 2 : 3 * d + 3, columns]
            lead_half[rows, 0:width] = (mass * (velocity * weight + first * slope)).astype(jnp.bfloat16)
            lead_half[rows, width : 2 * width] = (second * weight).astype(jnp.bfloat16)
            lead_half[rows, 2 * width : 3 * width] = (third * weight).astype(jnp.bfloat16)
        total = lax.dot_general(
            lead_half[...],
            plane_half[...],
            (((1,), (1,)), ((), ())),
            preferred_element_type=jnp.float32,
        )
        deposits_ref[place_ref[block]] = total.astype(jnp.bfloat16)

    @pl.loop(0, STEP_BLOCKS // 2)
    def _(pair):
        one_block(2 * pair, 0)
        one_block(2 * pair + 1, 1)


def deposit_all(mass, velocity, affine, cell, fraction, owner, slot, count, groups, capacity):
    blocks = owner.shape[0]
    width = mass.shape[0] // blocks
    columns = STEP_BLOCKS * width
    slots = groups * capacity

    def lanes(rows):
        return pl.BlockSpec((rows, columns), lambda i, *_: (0, i))

    return pl.pallas_call(
        functools.partial(deposit_kernel, capacity=capacity, width=width),
        grid_spec=pltpu.PrefetchScalarGridSpec(
            num_scalar_prefetch=3,
            grid=(blocks // STEP_BLOCKS,),
            in_specs=[lanes(1), lanes(3), lanes(9), lanes(3), lanes(3)],
            out_specs=[
                pl.BlockSpec((slots, 4 * EDGE, PLANE), lambda i, *_: (0, 0, 0)),
                pl.BlockSpec(memory_space=pltpu.SMEM),
                pl.BlockSpec(memory_space=pltpu.SMEM),
            ],
            scratch_shapes=[
                pltpu.SMEM((groups,), jnp.int32),
                pltpu.VMEM((2, 2 * EDGE, width), jnp.float32),
                pltpu.VMEM((2, PLANE, 3 * width), jnp.bfloat16),
                pltpu.VMEM((2, 4 * EDGE, 3 * width), jnp.bfloat16),
            ],
        ),
        out_shape=[
            jax.ShapeDtypeStruct((slots, 4 * EDGE, PLANE), jnp.bfloat16),
            jax.ShapeDtypeStruct((blocks,), jnp.int32),
            jax.ShapeDtypeStruct((slots,), jnp.int32),
        ],
        compiler_params=pltpu.CompilerParams(
            dimension_semantics=("arbitrary",), vmem_limit_bytes=40 << 20
        ),
        cost_estimate=pl.CostEstimate(
            flops=2 * blocks * 64 * PLANE * 3 * width, bytes_accessed=7 << 20, transcendentals=0
        ),
        name="deposit",
    )(owner, slot, count, mass.reshape(1, -1), velocity, affine, cell, fraction)


def update_kernel(tiles_ref, arrived_ref, drag_ref, velocity_ref, returned_ref, sums_ref, rounded_ref):
    slots = arrived_ref.shape[0]
    tiles = drag_ref.shape[0]
    sums_ref[...] = jnp.zeros_like(sums_ref)

    @pl.loop(0, slots)
    def _(slot):
        tile = tiles_ref[slot]

        @pl.when(tile >= 0)
        def _():
            sums_ref[tile] = sums_ref[tile] + arrived_ref[slot].astype(jnp.float32)

    @pl.loop(0, tiles)
    def _(tile):
        mass = sums_ref[tile, 0:EDGE, :] + drag_ref[tile]
        for d in range(3):
            rows = slice(d * EDGE, (d + 1) * EDGE)
            value = sums_ref[tile, (d + 1) * EDGE : (d + 2) * EDGE, :] / mass
            velocity_ref[tile, rows, :] = value
            rounded_ref[tile, rows, :] = value.astype(jnp.bfloat16)

    @pl.loop(0, slots)
    def _(slot):
        returned_ref[slot] = rounded_ref[jnp.maximum(tiles_ref[slot], 0)]


def update_grid(arrived, arrived_tiles, drag):
    slots = arrived.shape[0]
    tiles = drag.shape[0]
    whole = pl.BlockSpec(memory_space=pltpu.VMEM)
    return pl.pallas_call(
        update_kernel,
        in_specs=[pl.BlockSpec(memory_space=pltpu.SMEM), whole, whole],
        out_specs=[whole, whole],
        out_shape=[
            jax.ShapeDtypeStruct((tiles, 3 * EDGE, PLANE), jnp.float32),
            jax.ShapeDtypeStruct((slots, 3 * EDGE, PLANE), jnp.bfloat16),
        ],
        scratch_shapes=[
            pltpu.VMEM((tiles, 4 * EDGE, PLANE), jnp.float32),
            pltpu.VMEM((tiles, 3 * EDGE, PLANE), jnp.bfloat16),
        ],
        compiler_params=pltpu.CompilerParams(vmem_limit_bytes=40 << 20),
        cost_estimate=pl.CostEstimate(flops=1 << 24, bytes_accessed=8 << 20, transcendentals=0),
        name="update",
    )(arrived_tiles, arrived, drag)


def sample_kernel(
    place_ref,
    count_ref,
    cell_ref,
    fraction_ref,
    returned_ref,
    velocity_ref,
    affine_ref,
    rows_ref,
    plane_ref,
    *,
    width,
):
    step = pl.program_id(0)

    def one_block(local, half):
        block = step * STEP_BLOCKS + local
        columns = pl.ds(pl.multiple_of(local * width, width), width)
        rows_half, plane_half = rows_ref.at[half], plane_ref.at[half]
        fill_planes(cell_ref, fraction_ref, columns, rows_half, plane_half)
        weight, slope = stencil(cell_ref, fraction_ref, 0, columns)
        moments = jnp.dot(
            returned_ref[place_ref[block]], plane_half[...], preferred_element_type=jnp.float32
        )
        lane = lax.broadcasted_iota(jnp.int32, (1, width), 1)
        present = lane < count_ref[block]

        def gather(d, part, factor):
            moment = moments[d * EDGE : (d + 1) * EDGE, part * width : (part + 1) * width]
            total = jnp.sum(factor * moment, axis=0, keepdims=True)
            return jnp.where(present, total, 0.0)

        for d in range(3):
            velocity_ref[d : d + 1, columns] = gather(d, 0, weight)
            affine_ref[3 * d : 3 * d + 1, columns] = 4.0 * gather(d, 0, slope)
            affine_ref[3 * d + 1 : 3 * d + 2, columns] = 4.0 * gather(d, 1, weight)
            affine_ref[3 * d + 2 : 3 * d + 3, columns] = 4.0 * gather(d, 2, weight)

    @pl.loop(0, STEP_BLOCKS // 2)
    def _(pair):
        one_block(2 * pair, 0)
        one_block(2 * pair + 1, 1)


def sample_all(place, count, cell, fraction, returned):
    blocks = count.shape[0]
    width = cell.shape[1] // blocks
    columns = STEP_BLOCKS * width

    def lanes(rows):
        return pl.BlockSpec((rows, columns), lambda i, *_: (0, i))

    return pl.pallas_call(
        functools.partial(sample_kernel, width=width),
        grid_spec=pltpu.PrefetchScalarGridSpec(
            num_scalar_prefetch=2,
            grid=(blocks // STEP_BLOCKS,),
            in_specs=[lanes(3), lanes(3), pl.BlockSpec(returned.shape, lambda i, *_: (0, 0, 0))],
            out_specs=[lanes(3), lanes(9)],
            scratch_shapes=[
                pltpu.VMEM((2, 2 * EDGE, width), jnp.float32),
                pltpu.VMEM((2, PLANE, 3 * width), jnp.bfloat16),
            ],
        ),
        out_shape=[
            jax.ShapeDtypeStruct((3, cell.shape[1]), jnp.float32),
            jax.ShapeDtypeStruct((9, cell.shape[1]), jnp.float32),
        ],
        compiler_params=pltpu.CompilerParams(
            dimension_semantics=("arbitrary",), vmem_limit_bytes=40 << 20
        ),
        cost_estimate=pl.CostEstimate(
            flops=2 * blocks * 48 * PLANE * 3 * width, bytes_accessed=7 << 20, transcendentals=0
        ),
        name="sample",
    )(place, count, cell, fraction, returned)


def per_device(
    particle_mass,
    particle_velocity,
    particle_affine,
    particle_cell,
    particle_fraction,
    block_owner,
    block_slot,
    block_count,
    cell_drag,
):
    axes = ("gy", "gz")
    groups = lax.axis_size(axes)
    blocks = block_count.shape[0]
    capacity = max(1, 2 * blocks // groups)
    tiles = cell_drag.shape[0]
    deposits, place, tile_ids = deposit_all(
        particle_mass,
        particle_velocity,
        particle_affine,
        particle_cell,
        particle_fraction,
        block_owner.reshape(-1),
        block_slot,
        block_count,
        groups,
        capacity,
    )
    arrived_tiles = lax.all_to_all(tile_ids, axes, split_axis=0, concat_axis=0, tiled=True)
    arrived = lax.all_to_all(deposits, axes, split_axis=0, concat_axis=0, tiled=True)
    drag = cell_drag.reshape(tiles, EDGE, PLANE)
    velocity, answers = update_grid(arrived, arrived_tiles, drag)
    returned = lax.all_to_all(answers, axes, split_axis=0, concat_axis=0, tiled=True)
    new_velocity, new_affine = sample_all(
        place, block_count, particle_cell, particle_fraction, returned
    )
    return (velocity.reshape(tiles, 3, -1), new_velocity, new_affine)


def solution(mesh):
    split = ("gx", "gy", "gz")
    return jax.shard_map(
        per_device,
        mesh=mesh,
        in_specs=(
            P(split),
            P(None, split),
            P(None, split),
            P(None, split),
            P(None, split),
            P(split, None),
            P(split),
            P(split),
            P(split, None),
        ),
        out_specs=(P(split, None, None), P(None, split), P(None, split)),
        check_vma=False,
    )
```

```python
import functools

import jax
import jax.numpy as jnp
from jax import lax
from jax.experimental import pallas as pl
from jax.experimental.pallas import tpu as pltpu
from jax.sharding import PartitionSpec as P

EDGE = 16
QUANT = 1024
PLANE = EDGE * EDGE
LANES = 128
CHUNK = 4
MESH = pl.DeviceIdType.MESH
STEP_BLOCKS = 8


def stencil(cell_ref, fraction_ref, axis, columns):
    cell = cell_ref[axis : axis + 1, columns].astype(jnp.float32)
    fraction = fraction_ref[axis : axis + 1, columns].astype(jnp.float32)
    position = cell + 0.5 + (fraction + 0.5) / QUANT
    node = lax.broadcasted_iota(jnp.int32, (EDGE, position.shape[1]), 0).astype(jnp.float32)
    offset = node - position
    magnitude = jnp.abs(offset)
    inner = 0.75 - magnitude * magnitude
    reach = jnp.maximum(1.5 - magnitude, 0.0)
    weight = jnp.where(magnitude < 0.5, inner, 0.5 * reach * reach)
    return weight, weight * offset


def fill_planes(cell_ref, fraction_ref, columns, rows_ref, plane_ref):
    width = rows_ref.shape[1]
    weight_y, slope_y = stencil(cell_ref, fraction_ref, 1, columns)
    weight_z, slope_z = stencil(cell_ref, fraction_ref, 2, columns)
    rows_ref[0:EDGE, :] = weight_y
    rows_ref[EDGE : 2 * EDGE, :] = slope_y
    for y in range(EDGE):
        rows = slice(y * EDGE, (y + 1) * EDGE)
        along = rows_ref[y : y + 1, :]
        tilt = rows_ref[EDGE + y : EDGE + y + 1, :]
        plane_ref[rows, 0:width] = (along * weight_z).astype(jnp.bfloat16)
        plane_ref[rows, width : 2 * width] = (tilt * weight_z).astype(jnp.bfloat16)
        plane_ref[rows, 2 * width : 3 * width] = (along * slope_z).astype(jnp.bfloat16)


def deposit_kernel(
    owner_ref,
    slot_ref,
    count_ref,
    mass_ref,
    velocity_ref,
    affine_ref,
    cell_ref,
    fraction_ref,
    deposits_ref,
    names_ref,
    place_ref,
    used_ref,
    rows_ref,
    plane_ref,
    lead_ref,
    *,
    capacity,
    width,
    columns_of,
):
    step = pl.program_id(0)
    groups = used_ref.shape[0]
    blocks = owner_ref.shape[0]

    @pl.when(step == 0)
    def _():
        deposits_ref[...] = jnp.zeros_like(deposits_ref)
        lead_ref[...] = jnp.zeros_like(lead_ref)
        names_ref[...] = jnp.full_like(names_ref, -1.0)

        @pl.loop(0, groups)
        def _(group):
            used_ref[group] = 0

        @pl.loop(0, blocks)
        def _(block):
            owner = owner_ref[block]
            rank = used_ref[owner]
            used_ref[owner] = rank + 1
            row = lax.rem(owner, columns_of) * (groups // columns_of) + lax.div(owner, columns_of)
            place = row * capacity + rank
            place_ref[block] = place
            name = lax.convert_element_type(slot_ref[block], jnp.float32)
            names_ref[pl.ds(place, 1), :] = jnp.full((1, names_ref.shape[1]), name, jnp.float32)

    def one_block(local, half):
        block = step * STEP_BLOCKS + local
        columns = pl.ds(pl.multiple_of(local * width, width), width)
        rows_half, plane_half, lead_half = rows_ref.at[half], plane_ref.at[half], lead_ref.at[half]
        fill_planes(cell_ref, fraction_ref, columns, rows_half, plane_half)
        weight, slope = stencil(cell_ref, fraction_ref, 0, columns)
        lane = lax.broadcasted_iota(jnp.int32, (1, width), 1)
        mass = jnp.where(lane < count_ref[block], mass_ref[0:1, columns], 0.0)
        lead_half[0:EDGE, 0:width] = (mass * weight).astype(jnp.bfloat16)
        for d in range(3):
            rows = slice((d + 1) * EDGE, (d + 2) * EDGE)
            velocity = velocity_ref[d : d + 1, columns]
            first = affine_ref[3 * d : 3 * d + 1, columns]
            second = mass * affine_ref[3 * d + 1 : 3 * d + 2, columns]
            third = mass * affine_ref[3 * d + 2 : 3 * d + 3, columns]
            lead_half[rows, 0:width] = (mass * (velocity * weight + first * slope)).astype(jnp.bfloat16)
            lead_half[rows, width : 2 * width] = (second * weight).astype(jnp.bfloat16)
            lead_half[rows, 2 * width : 3 * width] = (third * weight).astype(jnp.bfloat16)
        total = lax.dot_general(
            lead_half[...],
            plane_half[...],
            (((1,), (1,)), ((), ())),
            preferred_element_type=jnp.float32,
        )
        deposits_ref[place_ref[block]] = total.astype(jnp.bfloat16)

    @pl.loop(0, STEP_BLOCKS // 2)
    def _(pair):
        one_block(2 * pair, 0)
        one_block(2 * pair + 1, 1)


def deposit_all(mass, velocity, affine, cell, fraction, owner, slot, count, groups, capacity, columns_of):
    blocks = owner.shape[0]
    width = mass.shape[0] // blocks
    columns = STEP_BLOCKS * width
    slots = groups * capacity

    def lanes(rows):
        return pl.BlockSpec((rows, columns), lambda i, *_: (0, i))

    return pl.pallas_call(
        functools.partial(
            deposit_kernel, capacity=capacity, width=width, columns_of=columns_of
        ),
        grid_spec=pltpu.PrefetchScalarGridSpec(
            num_scalar_prefetch=3,
            grid=(blocks // STEP_BLOCKS,),
            in_specs=[lanes(1), lanes(3), lanes(9), lanes(3), lanes(3)],
            out_specs=[
                pl.BlockSpec((slots, 4 * EDGE, PLANE), lambda i, *_: (0, 0, 0)),
                pl.BlockSpec((slots, LANES), lambda i, *_: (0, 0)),
                pl.BlockSpec(memory_space=pltpu.SMEM),
            ],
            scratch_shapes=[
                pltpu.SMEM((groups,), jnp.int32),
                pltpu.VMEM((2, 2 * EDGE, width), jnp.float32),
                pltpu.VMEM((2, PLANE, 3 * width), jnp.bfloat16),
                pltpu.VMEM((2, 4 * EDGE, 3 * width), jnp.bfloat16),
            ],
        ),
        out_shape=[
            jax.ShapeDtypeStruct((slots, 4 * EDGE, PLANE), jnp.bfloat16),
            jax.ShapeDtypeStruct((slots, LANES), jnp.float32),
            jax.ShapeDtypeStruct((blocks,), jnp.int32),
        ],
        compiler_params=pltpu.CompilerParams(
            dimension_semantics=("arbitrary",), vmem_limit_bytes=40 << 20
        ),
        cost_estimate=pl.CostEstimate(
            flops=2 * blocks * 64 * PLANE * 3 * width, bytes_accessed=7 << 20, transcendentals=0
        ),
        name="deposit",
    )(owner, slot, count, mass.reshape(1, -1), velocity, affine, cell, fraction)


def exchange_kernel(
    deposits_ref,
    names_ref,
    drag_ref,
    velocity_ref,
    back_ref,
    slot_in,
    name_in,
    relay,
    part_out,
    part_in,
    own_names,
    table,
    own_sum,
    grid_all,
    reply,
    relay_back,
    name_send,
    name_recv,
    out_send,
    out_recv,
    part_send,
    part_recv,
    grid_send,
    grid_recv,
    back_send,
    back_recv,
):
    side, ring, capacity = deposits_ref.shape[:3]
    tiles = drag_ref.shape[0]
    chunks = tiles // CHUNK
    half = capacity // 2
    steps = ring // 2
    g, q = lax.axis_index("gy"), lax.axis_index("gz")
    q_up, q_down, q_far = lax.rem(q + 1, side), lax.rem(q + side - 1, side), lax.rem(q + 2, side)
    up, down, far = {"gz": q_up}, {"gz": q_down}, {"gz": q_far}
    along = ({"gy": lax.rem(g + 1, ring)}, {"gy": lax.rem(g + ring - 1, ring)})

    def at(delta):
        return lax.rem(g + delta + ring, ring)

    def copy(source, target, send, recv, device):
        return pltpu.make_async_remote_copy(
            src_ref=source,
            dst_ref=target,
            send_sem=send,
            recv_sem=recv,
            device_id=device,
            device_id_type=MESH,
        )

    barrier = pltpu.get_barrier_semaphore()
    peers = (up, down, far) + along
    for peer in peers:
        pl.semaphore_signal(barrier, inc=1, device_id=peer, device_id_type=MESH)
    pl.semaphore_wait(barrier, len(peers))

    name_copies = [
        copy(names_ref.at[there], name_in.at[k], name_send.at[k], name_recv.at[k], device)
        for k, (there, device) in enumerate(((q_up, up), (q_down, down), (q_far, far)))
    ]
    for item in name_copies:
        item.start()

    order = [(4, None, 0), (3, 0, 1), (-3, 1, 1), (2, 0, 2), (-2, 1, 2), (1, 0, 3), (-1, 1, 3), (0, None, 4)]
    owners = [at(delta) for delta, _, _ in order]

    def outward(i):
        o = owners[i]
        return [
            copy(deposits_ref.at[q_up, o], slot_in.at[0, o], out_send.at[i, 0], out_recv.at[i, 0], up),
            copy(deposits_ref.at[q_down, o], slot_in.at[1, o], out_send.at[i, 1], out_recv.at[i, 1], down),
            copy(
                deposits_ref.at[q_far, o, pl.ds(0, half)],
                relay.at[0, o],
                out_send.at[i, 2],
                out_recv.at[i, 2],
                up,
            ),
            copy(
                deposits_ref.at[q_far, o, pl.ds(half, half)],
                relay.at[1, o],
                out_send.at[i, 3],
                out_recv.at[i, 3],
                down,
            ),
            copy(
                relay.at[0, o],
                slot_in.at[2, o, pl.ds(0, half)],
                out_send.at[i, 4],
                out_recv.at[i, 4],
                up,
            ),
            copy(
                relay.at[1, o],
                slot_in.at[2, o, pl.ds(half, half)],
                out_send.at[i, 5],
                out_recv.at[i, 5],
                down,
            ),
        ]

    out = [outward(i) for i in range(ring)]

    def first_hop(i):
        if i < ring:
            for item in out[i][:4]:
                item.start()

    def second_hop(i):
        if i < ring:
            for k in (0, 1):
                out[i][2 + k].wait_recv()
                out[i][4 + k].start()

    def part_copy(way, e, c):
        rows = pl.ds(c * CHUNK, CHUNK)
        return copy(
            part_out.at[way, e, rows],
            part_in.at[way, e, rows],
            part_send.at[way, e, c],
            part_recv.at[way, e, c],
            along[way],
        )

    def prepare(i):
        o = owners[i]
        for role in range(4):
            source = names_ref.at[q] if role == 3 else name_in.at[role]
            for r in range(capacity):
                row = role * capacity + r
                own_names[row : row + 1, :] = source[pl.ds(o * capacity + r, 1), :]
        named = own_names[...]
        for t in range(tiles):
            table[i, t] = jnp.where(named == float(t), 1.0, 0.0)

    def add_up(i, c, incoming, put):
        o = owners[i]

        @pl.loop(0, 4)
        def _(d):
            rows = pl.ds(pl.multiple_of(d * EDGE, EDGE), EDGE)
            sums = [None] * CHUNK
            for role in range(4):
                for r in range(capacity):
                    source = deposits_ref.at[q, o, r] if role == 3 else slot_in.at[role, o, r]
                    value = source[rows, :].astype(jnp.float32)
                    row = role * capacity + r
                    for t in range(CHUNK):
                        factor = table[i, c * CHUNK + t, row : row + 1, :]
                        term = jnp.concatenate([factor, factor], axis=1) * value
                        sums[t] = term if sums[t] is None else sums[t] + term
            for t in range(CHUNK):
                total = sums[t]
                for way, e in incoming:
                    total = total + part_in[way, e, c * CHUNK + t, rows, :].astype(jnp.float32)
                put(c, t, rows, total)

    def send_parts(i, way, e, first, last, incoming):
        @pl.loop(first, last)
        def _(k):
            c = lax.rem(k + way * (chunks // 2), chunks)
            for w, before in incoming:
                part_copy(w, before, c).wait_recv()

            def put(c, t, rows, total):
                part_out[way, e, c * CHUNK + t, rows, :] = total.astype(jnp.bfloat16)

            add_up(i, c, incoming, put)
            part_copy(way, e, c).start()

    first_hop(0)
    first_hop(1)
    for item in name_copies:
        item.wait_recv()
    second_hop(0)
    first_hop(2)
    for i, (_, way, e) in enumerate(order):
        second_hop(i + 1)
        first_hop(i + 3)
        prepare(i)
        for k in (0, 1, 4, 5):
            out[i][k].wait_recv()
        if e == 0:
            send_parts(i, 0, 0, 0, chunks // 2, ())
            send_parts(i, 1, 0, 0, chunks // 2, ())
        elif e == 1:
            send_parts(i, way, e, 0, chunks // 2, ((way, 0),))
            send_parts(i, way, e, chunks // 2, chunks, ())
        elif e < steps:
            send_parts(i, way, e, 0, chunks, ((way, e - 1),))

    def grid_copy(way, e, c):
        o = at(-e) if way == 0 else at(e)
        rows = pl.ds(c * CHUNK, CHUNK)
        return copy(
            grid_all.at[o, rows],
            grid_all.at[o, rows],
            grid_send.at[way, e, c],
            grid_recv.at[way, e, c],
            along[way],
        )

    @pl.loop(0, chunks)
    def _(c):
        for way in (0, 1):
            part_copy(way, steps - 1, c).wait_recv()

        def put(c, t, rows, total):
            own_sum[t, rows, :] = total

        add_up(ring - 1, c, ((0, steps - 1), (1, steps - 1)), put)
        for t in range(CHUNK):
            tile = c * CHUNK + t
            mass = own_sum[t, 0:EDGE, :] + drag_ref[tile]
            for d in range(3):
                rows = slice(d * EDGE, (d + 1) * EDGE)
                value = own_sum[t, (d + 1) * EDGE : (d + 2) * EDGE, :] / mass
                velocity_ref[tile, rows, :] = value
                grid_all[g, tile, rows, :] = value.astype(jnp.bfloat16)
        for way in (0, 1):
            grid_copy(way, 0, c).start()

    def inward(i):
        o = owners[i]
        return [
            copy(reply.at[1, o], back_ref.at[q, o], back_send.at[i, 0], back_recv.at[i, 0], up),
            copy(reply.at[0, o], back_ref.at[q, o], back_send.at[i, 1], back_recv.at[i, 1], down),
            copy(
                reply.at[2, o, pl.ds(0, half)],
                relay_back.at[0, o],
                back_send.at[i, 2],
                back_recv.at[i, 2],
                up,
            ),
            copy(
                reply.at[2, o, pl.ds(half, half)],
                relay_back.at[1, o],
                back_send.at[i, 3],
                back_recv.at[i, 3],
                down,
            ),
            copy(
                relay_back.at[0, o],
                back_ref.at[q_down, o, pl.ds(0, half)],
                back_send.at[i, 4],
                back_recv.at[i, 4],
                up,
            ),
            copy(
                relay_back.at[1, o],
                back_ref.at[q_up, o, pl.ds(half, half)],
                back_send.at[i, 5],
                back_recv.at[i, 5],
                down,
            ),
        ]

    replies = [inward(i) for i in range(ring)]

    def pick(i, role, r, target):
        o = owners[i]
        row = role * capacity + r
        total = None
        for t in range(tiles):
            factor = jnp.broadcast_to(table[i, t, pl.ds(row, 1), :], (EDGE, LANES)).astype(jnp.bfloat16)
            factor = jnp.concatenate([factor, factor], axis=1)
            factor = jnp.concatenate([factor] * 3, axis=0)
            term = factor * grid_all[o, t]
            total = term if total is None else total + term
        target[...] = total

    def answer(i):
        o = owners[i]

        @pl.loop(0, capacity)
        def _(r):
            for role in range(3):
                pick(i, role, r, reply.at[role, o, r])
            pick(i, 3, r, back_ref.at[q, o, r])

        for item in replies[i][:4]:
            item.start()

    def pass_back(i):
        for k in (0, 1):
            replies[i][2 + k].wait_recv()
            replies[i][4 + k].start()

    answer(ring - 1)
    waiting = [ring - 1]
    for e in range(steps):
        last = e == steps - 1

        def take(first, stop):
            @pl.loop(first, stop)
            def _(k):
                for way in (0, 1):
                    c = lax.rem(k + way * (chunks // 2), chunks)
                    grid_copy(way, e, c).wait_recv()
                    if e + 1 < steps - 1:
                        grid_copy(way, e + 1, c).start()

        def take_final(first, stop):
            @pl.loop(first, stop)
            def _(k):
                for way in (0, 1):
                    c = lax.rem(k + way * (chunks // 2), chunks)
                    grid_copy(way, e, c).wait_recv()
                    grid_copy(way, e + 1, c).start()

        if last:
            for i in waiting:
                pass_back(i)
            take(0, chunks // 2)
            now = [0]
        else:
            if e + 1 == steps - 1:
                take_final(0, chunks // 2)
            else:
                take(0, chunks // 2)
            for i in waiting:
                pass_back(i)
            take(chunks // 2, chunks)
            now = [ring - 2 - 2 * e, ring - 3 - 2 * e]
        for i in now:
            answer(i)
        waiting = now
    for i in waiting:
        pass_back(i)

    for i in range(ring):
        for k in (0, 1, 4, 5):
            replies[i][k].wait_recv()
    for item in name_copies:
        item.wait_send()
    for i in range(ring):
        for k in range(6):
            out[i][k].wait_send()
            replies[i][k].wait_send()
    for way in (0, 1):
        for e in range(1, steps):

            @pl.loop(0, chunks)
            def _(c):
                part_copy(way, e, c).wait_send()
                grid_copy(way, e - 1, c).wait_send()

        @pl.loop(0, chunks // 2)
        def _(k):
            c = k + way * (chunks // 2)
            part_copy(way, 0, c).wait_send()
            grid_copy(way, steps - 1, c).wait_send()


def exchange(deposits, names, drag):
    side, ring, capacity = deposits.shape[:3]
    tiles = drag.shape[0]
    steps = ring // 2
    chunks = tiles // CHUNK
    half = capacity // 2
    whole = pl.BlockSpec(memory_space=pltpu.VMEM)
    dma = pltpu.SemaphoreType.DMA
    block, answer = (4 * EDGE, PLANE), (3 * EDGE, PLANE)
    return pl.pallas_call(
        exchange_kernel,
        in_specs=[whole] * 3,
        out_specs=[whole] * 2,
        out_shape=[
            jax.ShapeDtypeStruct((tiles,) + answer, jnp.float32),
            jax.ShapeDtypeStruct((side, ring, capacity) + answer, jnp.bfloat16),
        ],
        scratch_shapes=[
            pltpu.VMEM((3, ring, capacity) + block, jnp.bfloat16),
            pltpu.VMEM((3,) + names.shape[1:], jnp.float32),
            pltpu.VMEM((2, ring, half) + block, jnp.bfloat16),
            pltpu.VMEM((2, steps, tiles) + block, jnp.bfloat16),
            pltpu.VMEM((2, steps, tiles) + block, jnp.bfloat16),
            pltpu.VMEM((4 * capacity, LANES), jnp.float32),
            pltpu.VMEM((ring, tiles, 4 * capacity, LANES), jnp.float32),
            pltpu.VMEM((CHUNK,) + block, jnp.float32),
            pltpu.VMEM((ring, tiles) + answer, jnp.bfloat16),
            pltpu.VMEM((3, ring, capacity) + answer, jnp.bfloat16),
            pltpu.VMEM((2, ring, half) + answer, jnp.bfloat16),
            dma((3,)),
            dma((3,)),
            dma((ring, 6)),
            dma((ring, 6)),
            dma((2, steps, chunks)),
            dma((2, steps, chunks)),
            dma((2, steps, chunks)),
            dma((2, steps, chunks)),
            dma((ring, 6)),
            dma((ring, 6)),
        ],
        compiler_params=pltpu.CompilerParams(
            collective_id=0, has_side_effects=True, vmem_limit_bytes=56 << 20
        ),
        cost_estimate=pl.CostEstimate(flops=1 << 26, bytes_accessed=8 << 20, transcendentals=0),
        name="exchange",
    )(deposits, names, drag)


def sample_kernel(
    place_ref,
    count_ref,
    cell_ref,
    fraction_ref,
    returned_ref,
    velocity_ref,
    affine_ref,
    rows_ref,
    plane_ref,
    *,
    width,
):
    step = pl.program_id(0)

    def one_block(local, half):
        block = step * STEP_BLOCKS + local
        columns = pl.ds(pl.multiple_of(local * width, width), width)
        rows_half, plane_half = rows_ref.at[half], plane_ref.at[half]
        fill_planes(cell_ref, fraction_ref, columns, rows_half, plane_half)
        weight, slope = stencil(cell_ref, fraction_ref, 0, columns)
        moments = jnp.dot(
            returned_ref[place_ref[block]], plane_half[...], preferred_element_type=jnp.float32
        )
        lane = lax.broadcasted_iota(jnp.int32, (1, width), 1)
        present = lane < count_ref[block]

        def gather(d, part, factor):
            moment = moments[d * EDGE : (d + 1) * EDGE, part * width : (part + 1) * width]
            total = jnp.sum(factor * moment, axis=0, keepdims=True)
            return jnp.where(present, total, 0.0)

        for d in range(3):
            velocity_ref[d : d + 1, columns] = gather(d, 0, weight)
            affine_ref[3 * d : 3 * d + 1, columns] = 4.0 * gather(d, 0, slope)
            affine_ref[3 * d + 1 : 3 * d + 2, columns] = 4.0 * gather(d, 1, weight)
            affine_ref[3 * d + 2 : 3 * d + 3, columns] = 4.0 * gather(d, 2, weight)

    @pl.loop(0, STEP_BLOCKS // 2)
    def _(pair):
        one_block(2 * pair, 0)
        one_block(2 * pair + 1, 1)


def sample_all(place, count, cell, fraction, returned):
    blocks = count.shape[0]
    width = cell.shape[1] // blocks
    columns = STEP_BLOCKS * width

    def lanes(rows):
        return pl.BlockSpec((rows, columns), lambda i, *_: (0, i))

    return pl.pallas_call(
        functools.partial(sample_kernel, width=width),
        grid_spec=pltpu.PrefetchScalarGridSpec(
            num_scalar_prefetch=2,
            grid=(blocks // STEP_BLOCKS,),
            in_specs=[lanes(3), lanes(3), pl.BlockSpec(returned.shape, lambda i, *_: (0, 0, 0))],
            out_specs=[lanes(3), lanes(9)],
            scratch_shapes=[
                pltpu.VMEM((2, 2 * EDGE, width), jnp.float32),
                pltpu.VMEM((2, PLANE, 3 * width), jnp.bfloat16),
            ],
        ),
        out_shape=[
            jax.ShapeDtypeStruct((3, cell.shape[1]), jnp.float32),
            jax.ShapeDtypeStruct((9, cell.shape[1]), jnp.float32),
        ],
        compiler_params=pltpu.CompilerParams(
            dimension_semantics=("arbitrary",), vmem_limit_bytes=40 << 20
        ),
        cost_estimate=pl.CostEstimate(
            flops=2 * blocks * 48 * PLANE * 3 * width, bytes_accessed=7 << 20, transcendentals=0
        ),
        name="sample",
    )(place, count, cell, fraction, returned)


def per_device(
    particle_mass,
    particle_velocity,
    particle_affine,
    particle_cell,
    particle_fraction,
    block_owner,
    block_slot,
    block_count,
    cell_drag,
):
    ring, side = lax.axis_size("gy"), lax.axis_size("gz")
    groups = ring * side
    blocks = block_count.shape[0]
    capacity = max(1, 2 * blocks // groups)
    tiles = cell_drag.shape[0]
    deposits, names, place = deposit_all(
        particle_mass,
        particle_velocity,
        particle_affine,
        particle_cell,
        particle_fraction,
        block_owner.reshape(-1),
        block_slot,
        block_count,
        groups,
        capacity,
        side,
    )
    velocity, back = exchange(
        deposits.reshape(side, ring, capacity, 4 * EDGE, PLANE),
        names.reshape(side, ring * capacity, LANES),
        cell_drag.reshape(tiles, EDGE, PLANE),
    )
    new_velocity, new_affine = sample_all(
        place,
        block_count,
        particle_cell,
        particle_fraction,
        back.reshape(groups * capacity, 3 * EDGE, PLANE),
    )
    return (velocity.reshape(tiles, 3, -1), new_velocity, new_affine)


def solution(mesh):
    split = ("gx", "gy", "gz")
    return jax.shard_map(
        per_device,
        mesh=mesh,
        in_specs=(
            P(split),
            P(None, split),
            P(None, split),
            P(None, split),
            P(None, split),
            P(split, None),
            P(split),
            P(split),
            P(split, None),
        ),
        out_specs=(P(split, None, None), P(None, split), P(None, split)),
        check_vma=False,
    )
```

```python
import jax
import jax.numpy as jnp
from jax import lax
from jax.experimental import pallas as pl
from jax.experimental.pallas import tpu as pltpu
from jax.sharding import PartitionSpec as P

EDGE = 16
QUANT = 1024
PLANE = EDGE * EDGE
LANES = 128
CHUNK = 4
MESH = pl.DeviceIdType.MESH
ORDER = ((4, None, 0), (3, 0, 1), (-3, 1, 1), (2, 0, 2), (-2, 1, 2), (1, 0, 3), (-1, 1, 3), (0, None, 4))


def stencil(cell, fraction):
    position = cell.astype(jnp.float32) + 0.5 + (fraction.astype(jnp.float32) + 0.5) / QUANT
    node = lax.broadcasted_iota(jnp.int32, (EDGE, position.shape[1]), 0).astype(jnp.float32)
    offset = node - position
    magnitude = jnp.abs(offset)
    inner = 0.75 - magnitude * magnitude
    reach = jnp.maximum(1.5 - magnitude, 0.0)
    weight = jnp.where(magnitude < 0.5, inner, 0.5 * reach * reach)
    return weight, weight * offset


def fill_planes(cell_ref, fraction_ref, columns, rows_ref, plane_ref):
    width = rows_ref.shape[1]
    weight_y, slope_y = stencil(cell_ref[1:2, columns], fraction_ref[1:2, columns])
    weight_z, slope_z = stencil(cell_ref[2:3, columns], fraction_ref[2:3, columns])
    rows_ref[0:EDGE, :] = weight_y
    rows_ref[EDGE : 2 * EDGE, :] = slope_y
    for y in range(EDGE):
        rows = slice(y * EDGE, (y + 1) * EDGE)
        along = rows_ref[y : y + 1, :]
        tilt = rows_ref[EDGE + y : EDGE + y + 1, :]
        plane_ref[rows, 0:width] = (along * weight_z).astype(jnp.bfloat16)
        plane_ref[rows, width : 2 * width] = (tilt * weight_z).astype(jnp.bfloat16)
        plane_ref[rows, 2 * width : 3 * width] = (along * slope_z).astype(jnp.bfloat16)


def plan_kernel(
    owner_ref,
    slot_ref,
    count_ref,
    block_ref,
    place_ref,
    row_ref,
    filled_ref,
    source_ref,
    names_ref,
    stages_ref,
    used_ref,
    raw_ref,
    *,
    ring,
    side,
    capacity,
):
    blocks = owner_ref.shape[0]
    slots = ring * side * capacity
    g = lax.axis_index("gy")
    names_ref[...] = jnp.full_like(names_ref, -1.0)
    for key in range(ring * side):
        used_ref[key] = 0
    for slot in range(slots):
        raw_ref[slot] = -1

    @pl.loop(0, blocks)
    def _(block):
        owner = owner_ref[block]
        column, tall = lax.rem(owner, side), lax.div(owner, side)
        ahead = lax.rem(tall - g + ring, ring)
        distance = jnp.minimum(ahead, ring - ahead)
        stage = ring - 2 * distance - jnp.where(ahead < ring // 2, 1, 0)
        key = stage * side + column
        rank = used_ref[key]
        used_ref[key] = rank + 1
        raw_ref[key * capacity + rank] = block
        name = lax.convert_element_type(slot_ref[block], jnp.float32)
        line = (column * ring + stage) * capacity + rank
        names_ref[pl.ds(line, 1), :] = jnp.full((1, LANES), name, jnp.float32)

    def sweep(slot, found):
        block = raw_ref[slot]
        here = block >= 0
        block = jnp.maximum(block, 0)
        source_ref[slot] = jnp.where(here, found, 0)
        block_ref[found] = block
        filled_ref[found] = count_ref[block]
        row_ref[found] = lax.rem(slot, side * capacity)
        place_ref[jnp.where(here, block, blocks)] = found
        stage = lax.convert_element_type(lax.div(slot, side * capacity), jnp.float32)
        stages_ref[pl.ds(found, 1), :] = jnp.full((1, LANES), stage, jnp.float32)
        return found + jnp.where(here, 1, 0)

    lax.fori_loop(0, slots, sweep, 0)


def make_plan(owner, slot, count, ring, side, capacity):
    blocks = owner.shape[0]
    slots = ring * side * capacity
    scalars = pl.BlockSpec(memory_space=pltpu.SMEM)
    listed = jax.ShapeDtypeStruct((blocks + 8,), jnp.int32)

    def kernel(*refs):
        plan_kernel(*refs, ring=ring, side=side, capacity=capacity)

    return pl.pallas_call(
        kernel,
        in_specs=[scalars] * 3,
        out_specs=[scalars] * 5 + [pl.BlockSpec(memory_space=pltpu.VMEM)] * 2,
        out_shape=[listed] * 4
        + [
            jax.ShapeDtypeStruct((slots,), jnp.int32),
            jax.ShapeDtypeStruct((slots, LANES), jnp.float32),
            jax.ShapeDtypeStruct((blocks + 8, LANES), jnp.float32),
        ],
        scratch_shapes=[pltpu.SMEM((ring * side,), jnp.int32), pltpu.SMEM((slots,), jnp.int32)],
        name="plan",
    )(owner, slot, count)


def transfer_kernel(
    block_ref,
    place_ref,
    row_ref,
    filled_ref,
    source_ref,
    names_ref,
    stages_ref,
    mass_hbm,
    motion_hbm,
    affine_hbm,
    cell_hbm,
    fraction_hbm,
    drag_hbm,
    velocity_ref,
    new_velocity_ref,
    new_affine_ref,
    mass_ref,
    motion_ref,
    affine_ref,
    cell_ref,
    fraction_ref,
    drag_ref,
    packed,
    slots_out,
    slot_in,
    name_in,
    relay,
    part_out,
    part_in,
    own_names,
    table,
    own_sum,
    grid_all,
    reply,
    relay_back,
    rows_ref,
    plane_ref,
    lead_ref,
    found_velocity,
    found_affine,
    load_sem,
    name_send,
    name_recv,
    out_send,
    out_recv,
    part_send,
    part_recv,
    grid_send,
    grid_recv,
    back_send,
    back_recv,
    *back,
):
    ring, side, capacity = slots_out.shape[:3]
    tiles = drag_ref.shape[0]
    chunks = tiles // CHUNK
    half = capacity // 2
    steps = ring // 2
    blocks = packed.shape[0]
    batch = side * capacity
    width = rows_ref.shape[2]
    g, q = lax.axis_index("gy"), lax.axis_index("gz")
    q_up, q_down, q_far = lax.rem(q + 1, side), lax.rem(q + side - 1, side), lax.rem(q + 2, side)
    up, down, far = {"gz": q_up}, {"gz": q_down}, {"gz": q_far}
    along = ({"gy": lax.rem(g + 1, ring)}, {"gy": lax.rem(g + ring - 1, ring)})
    owners = [lax.rem(g + delta + ring, ring) for delta, _, _ in ORDER]

    loads = [
        pltpu.make_async_copy(source, target, load_sem.at[k])
        for k, (source, target) in enumerate(
            (
                (cell_hbm, cell_ref),
                (fraction_hbm, fraction_ref),
                (mass_hbm, mass_ref),
                (motion_hbm, motion_ref),
                (affine_hbm, affine_ref),
                (drag_hbm, drag_ref),
            )
        )
    ]
    for item in loads:
        item.start()

    def copy(source, target, send, recv, device):
        return pltpu.make_async_remote_copy(
            src_ref=source,
            dst_ref=target,
            send_sem=send,
            recv_sem=recv,
            device_id=device,
            device_id_type=MESH,
        )

    barrier = pltpu.get_barrier_semaphore()
    peers = (up, down, far) + along
    for peer in peers:
        pl.semaphore_signal(barrier, inc=1, device_id=peer, device_id_type=MESH)
    lead_ref[...] = jnp.zeros_like(lead_ref)
    for item in loads:
        item.wait()

    def deposit(k, part):
        block = block_ref[k]
        columns = pl.ds(block * width, width)
        plane, lead = plane_ref.at[part], lead_ref.at[part]
        fill_planes(cell_ref, fraction_ref, columns, rows_ref.at[part], plane)
        weight, slope = stencil(cell_ref[0:1, columns], fraction_ref[0:1, columns])
        lane = lax.broadcasted_iota(jnp.int32, (1, width), 1)
        mass = jnp.where(lane < filled_ref[k], mass_ref[0:1, columns], 0.0)
        lead[0:EDGE, 0:width] = (mass * weight).astype(jnp.bfloat16)
        for d in range(3):
            rows = slice((d + 1) * EDGE, (d + 2) * EDGE)
            motion = motion_ref[d : d + 1, columns]
            first = affine_ref[3 * d : 3 * d + 1, columns]
            second = mass * affine_ref[3 * d + 1 : 3 * d + 2, columns]
            third = mass * affine_ref[3 * d + 2 : 3 * d + 3, columns]
            lead[rows, 0:width] = (mass * (motion * weight + first * slope)).astype(jnp.bfloat16)
            lead[rows, width : 2 * width] = (second * weight).astype(jnp.bfloat16)
            lead[rows, 2 * width : 3 * width] = (third * weight).astype(jnp.bfloat16)
        total = lax.dot_general(
            lead[...], plane[...], (((1,), (1,)), ((), ())), preferred_element_type=jnp.float32
        )
        packed[k] = total.astype(jnp.bfloat16)

    def deposit_batch(b):
        @pl.loop(0, batch // 2)
        def _(pair):
            deposit(b * batch + 2 * pair, 0)
            deposit(b * batch + 2 * pair + 1, 1)

    def spread(row, count):
        factor = jnp.broadcast_to(row, (EDGE, LANES)).astype(jnp.bfloat16)
        factor = jnp.concatenate([factor, factor], axis=1)
        return jnp.concatenate([factor] * count, axis=0)

    def assemble(i):
        for column in range(side):

            @pl.loop(0, capacity)
            def _(r):
                place = source_ref[(i * side + column) * capacity + r]
                name = names_ref[column, pl.ds(i * capacity + r, 1), :]
                slots_out[i, column, r] = packed[place] * spread(jnp.where(name >= 0.0, 1.0, 0.0), 4)

    name_copies = [
        copy(names_ref.at[there], name_in.at[k], name_send.at[k], name_recv.at[k], device)
        for k, (there, device) in enumerate(((q_up, up), (q_down, down), (q_far, far)))
    ]

    def outward(i):
        return [
            copy(slots_out.at[i, q_up], slot_in.at[0, i], out_send.at[i, 0], out_recv.at[i, 0], up),
            copy(slots_out.at[i, q_down], slot_in.at[1, i], out_send.at[i, 1], out_recv.at[i, 1], down),
            copy(
                slots_out.at[i, q_far, pl.ds(0, half)],
                relay.at[0, i],
                out_send.at[i, 2],
                out_recv.at[i, 2],
                up,
            ),
            copy(
                slots_out.at[i, q_far, pl.ds(half, half)],
                relay.at[1, i],
                out_send.at[i, 3],
                out_recv.at[i, 3],
                down,
            ),
            copy(
                relay.at[0, i],
                slot_in.at[2, i, pl.ds(0, half)],
                out_send.at[i, 4],
                out_recv.at[i, 4],
                up,
            ),
            copy(
                relay.at[1, i],
                slot_in.at[2, i, pl.ds(half, half)],
                out_send.at[i, 5],
                out_recv.at[i, 5],
                down,
            ),
        ]

    out = [outward(i) for i in range(ring)]

    def first_hop(i):
        if i < ring:
            for k in (2, 3, 0, 1):
                out[i][k].start()

    def second_hop(i):
        if i < ring:
            for k in (0, 1):
                out[i][2 + k].wait_recv()
                out[i][4 + k].start()

    def part_copy(way, e, c):
        rows = pl.ds(c * CHUNK, CHUNK)
        return copy(
            part_out.at[way, e, rows],
            part_in.at[way, e, rows],
            part_send.at[way, e, c],
            part_recv.at[way, e, c],
            along[way],
        )

    def prepare(i):
        for role in range(4):
            source = names_ref.at[q] if role == 3 else name_in.at[role]
            lines = slice(role * capacity, (role + 1) * capacity)
            own_names[lines, :] = source[i * capacity : (i + 1) * capacity, :]
        named = own_names[...]
        for t in range(tiles):
            table[i, t] = jnp.where(named == float(t), 1.0, 0.0)

    def add_up(i, c, incoming, put):
        @pl.loop(0, 4)
        def _(d):
            rows = pl.ds(pl.multiple_of(d * EDGE, EDGE), EDGE)
            sums = [None] * CHUNK
            for role in range(4):
                for r in range(capacity):
                    source = slots_out.at[i, q, r] if role == 3 else slot_in.at[role, i, r]
                    value = source[rows, :].astype(jnp.float32)
                    line = role * capacity + r
                    for t in range(CHUNK):
                        factor = table[i, c * CHUNK + t, line : line + 1, :]
                        term = jnp.concatenate([factor, factor], axis=1) * value
                        sums[t] = term if sums[t] is None else sums[t] + term
            for t in range(CHUNK):
                total = sums[t]
                for way, e in incoming:
                    total = total + part_in[way, e, c * CHUNK + t, rows, :].astype(jnp.float32)
                put(c, t, rows, total)

    def send_parts(i, way, e, first, last, incoming):
        @pl.loop(first, last)
        def _(k):
            c = lax.rem(k + way * (chunks // 2), chunks)
            for w, before in incoming:
                part_copy(w, before, c).wait_recv()

            def put(c, t, rows, total):
                part_out[way, e, c * CHUNK + t, rows, :] = total.astype(jnp.bfloat16)

            add_up(i, c, incoming, put)
            part_copy(way, e, c).start()

    def gather(i):
        _, way, e = ORDER[i]
        prepare(i)
        for k in (0, 1, 4, 5):
            out[i][k].wait_recv()
        if e == 0:
            send_parts(i, 0, 0, 0, chunks // 2, ())
            send_parts(i, 1, 0, 0, chunks // 2, ())
        elif e == 1:
            send_parts(i, way, e, 0, chunks // 2, ((way, 0),))
            send_parts(i, way, e, chunks // 2, chunks, ())
        elif e < steps:
            send_parts(i, way, e, 0, chunks, ((way, e - 1),))

    deposit_batch(0)
    assemble(0)
    pl.semaphore_wait(barrier, len(peers))
    for item in name_copies:
        item.start()
    first_hop(0)
    deposit_batch(1)
    assemble(1)
    second_hop(0)
    first_hop(1)
    for item in name_copies:
        item.wait_recv()
    deposit_batch(2)
    assemble(2)
    second_hop(1)
    first_hop(2)
    gather(0)
    deposit_batch(3)
    for i in range(3, ring):
        assemble(i)
    first_hop(3)
    for i in range(1, ring):
        second_hop(i + 1)
        first_hop(i + 3)
        gather(i)

    def grid_copy(way, e, c):
        o = lax.rem(g + (ring - e if way == 0 else e), ring)
        rows = pl.ds(c * CHUNK, CHUNK)
        return copy(
            grid_all.at[o, rows],
            grid_all.at[o, rows],
            grid_send.at[way, e, c],
            grid_recv.at[way, e, c],
            along[way],
        )

    @pl.loop(0, chunks)
    def _(c):
        for way in (0, 1):
            part_copy(way, steps - 1, c).wait_recv()

        def put(c, t, rows, total):
            own_sum[t, rows, :] = total

        add_up(ring - 1, c, ((0, steps - 1), (1, steps - 1)), put)
        for t in range(CHUNK):
            tile = c * CHUNK + t
            mass = own_sum[t, 0:EDGE, :] + drag_ref[tile]
            for d in range(3):
                rows = slice(d * EDGE, (d + 1) * EDGE)
                value = own_sum[t, (d + 1) * EDGE : (d + 2) * EDGE, :] / mass
                velocity_ref[tile, rows, :] = value
                grid_all[g, tile, rows, :] = value.astype(jnp.bfloat16)
        for way in (0, 1):
            grid_copy(way, 0, c).start()

    def inward(i):
        mine = pl.ds(q * capacity, capacity)
        return [
            copy(reply.at[1, i], back[i].at[mine], back_send.at[i, 0], back_recv.at[i, 0], up),
            copy(reply.at[0, i], back[i].at[mine], back_send.at[i, 1], back_recv.at[i, 1], down),
            copy(
                reply.at[2, i, pl.ds(0, half)],
                relay_back.at[0, i],
                back_send.at[i, 2],
                back_recv.at[i, 2],
                up,
            ),
            copy(
                reply.at[2, i, pl.ds(half, half)],
                relay_back.at[1, i],
                back_send.at[i, 3],
                back_recv.at[i, 3],
                down,
            ),
            copy(
                relay_back.at[0, i],
                back[i].at[pl.ds(q_down * capacity, half)],
                back_send.at[i, 4],
                back_recv.at[i, 4],
                up,
            ),
            copy(
                relay_back.at[1, i],
                back[i].at[pl.ds(q_up * capacity + half, half)],
                back_send.at[i, 5],
                back_recv.at[i, 5],
                down,
            ),
        ]

    replies = [inward(i) for i in range(ring)]

    def pick(i, role, r, target):
        o = owners[i]
        line = role * capacity + r
        total = None
        for t in range(tiles):
            term = spread(table[i, t, pl.ds(line, 1), :], 3) * grid_all[o, t]
            total = term if total is None else total + term
        target[...] = total

    def answer(i):
        @pl.loop(0, capacity)
        def _(r):
            for role in range(3):
                pick(i, role, r, reply.at[role, i, r])
            pick(i, 3, r, back[i].at[q * capacity + r])

        for k in (2, 3, 0, 1):
            replies[i][k].start()

    def pass_back(i):
        for k in (0, 1):
            replies[i][2 + k].wait_recv()
            replies[i][4 + k].start()

    def arrived(i):
        for k in (0, 1, 4, 5):
            replies[i][k].wait_recv()

    def sample(k, part, first):
        block = block_ref[k]
        stage, row = stages_ref[pl.ds(k, 1), :], row_ref[k]
        columns = pl.ds(block * width, width)
        plane = plane_ref.at[part]
        fill_planes(cell_ref, fraction_ref, columns, rows_ref.at[part], plane)
        weight, slope = stencil(cell_ref[0:1, columns], fraction_ref[0:1, columns])
        nodes = None
        for i in range(first, ring):
            term = spread(jnp.where(stage == float(i), 1.0, 0.0), 3) * back[i][row]
            nodes = term if nodes is None else nodes + term
        moments = jnp.dot(nodes, plane[...], preferred_element_type=jnp.float32)
        lane = lax.broadcasted_iota(jnp.int32, (1, width), 1)
        present = lane < filled_ref[k]

        def reduced(d, which, factor):
            moment = moments[d * EDGE : (d + 1) * EDGE, which * width : (which + 1) * width]
            total = jnp.sum(factor * moment, axis=0, keepdims=True)
            return jnp.where(present, total, 0.0)

        for d in range(3):
            found_velocity[k, d : d + 1, :] = reduced(d, 0, weight)
            found_affine[k, 3 * d : 3 * d + 1, :] = 4.0 * reduced(d, 0, slope)
            found_affine[k, 3 * d + 1 : 3 * d + 2, :] = 4.0 * reduced(d, 1, weight)
            found_affine[k, 3 * d + 2 : 3 * d + 3, :] = 4.0 * reduced(d, 2, weight)

    def sample_batch(b):
        @pl.loop(0, batch // 2)
        def _(pair):
            sample(b * batch + 2 * pair, 0, b)
            sample(b * batch + 2 * pair + 1, 1, b)

    def take(e, first, last, onward):
        @pl.loop(first, last)
        def _(k):
            for way in (0, 1):
                c = lax.rem(k + way * (chunks // 2), chunks)
                grid_copy(way, e, c).wait_recv()
                if onward:
                    grid_copy(way, e + 1, c).start()

    answer(7)
    take(0, 0, chunks // 2, True)
    pass_back(7)
    take(0, chunks // 2, chunks, True)
    answer(6)
    answer(5)
    take(1, 0, chunks // 2, True)
    pass_back(6)
    pass_back(5)
    take(1, chunks // 2, chunks, True)
    answer(4)
    answer(3)
    take(2, 0, chunks // 2, True)
    pass_back(4)
    pass_back(3)
    take(2, chunks // 2, chunks, False)
    answer(2)
    answer(1)
    for i in (7, 6, 5, 4, 3):
        arrived(i)
    sample_batch(3)
    take(3, 0, chunks // 2, False)
    answer(0)
    pass_back(2)
    pass_back(1)
    pass_back(0)
    arrived(2)
    sample_batch(2)
    arrived(1)
    sample_batch(1)
    arrived(0)
    sample_batch(0)

    @pl.loop(0, blocks)
    def _(block):
        columns = pl.ds(pl.multiple_of(block * width, width), width)
        place = place_ref[block]
        new_velocity_ref[:, columns] = found_velocity[place]
        new_affine_ref[:, columns] = found_affine[place]

    for item in name_copies:
        item.wait_send()
    for i in range(ring):
        for k in range(6):
            out[i][k].wait_send()
            replies[i][k].wait_send()
    for way in (0, 1):
        for e in range(1, steps):

            @pl.loop(0, chunks)
            def _(c):
                part_copy(way, e, c).wait_send()
                grid_copy(way, e - 1, c).wait_send()

        @pl.loop(0, chunks // 2)
        def _(k):
            c = k + way * (chunks // 2)
            part_copy(way, 0, c).wait_send()
            grid_copy(way, steps - 1, c).wait_send()


def transfer(plan, blocks, mass, motion, affine, cell, fraction, drag, ring, side, capacity):
    total = cell.shape[1]
    width = total // blocks
    tiles = drag.shape[0]
    steps = ring // 2
    chunks = tiles // CHUNK
    half = capacity // 2
    scalars = pl.BlockSpec(memory_space=pltpu.SMEM)
    whole = pl.BlockSpec(memory_space=pltpu.VMEM)
    outside = pl.BlockSpec(memory_space=pltpu.HBM)
    dma = pltpu.SemaphoreType.DMA
    block, answer = (4 * EDGE, PLANE), (3 * EDGE, PLANE)
    *lists, names, stages = plan
    return pl.pallas_call(
        transfer_kernel,
        in_specs=[scalars] * 5 + [whole] * 2 + [outside] * 6,
        out_specs=[whole] * 3,
        out_shape=[
            jax.ShapeDtypeStruct((tiles,) + answer, jnp.float32),
            jax.ShapeDtypeStruct((3, total), jnp.float32),
            jax.ShapeDtypeStruct((9, total), jnp.float32),
        ],
        scratch_shapes=[
            pltpu.VMEM((1, total), jnp.float32),
            pltpu.VMEM((3, total), jnp.float32),
            pltpu.VMEM((9, total), jnp.float32),
            pltpu.VMEM((3, total), jnp.int32),
            pltpu.VMEM((3, total), jnp.int32),
            pltpu.VMEM(drag.shape, jnp.float32),
            pltpu.VMEM((blocks,) + block, jnp.bfloat16),
            pltpu.VMEM((ring, side, capacity) + block, jnp.bfloat16),
            pltpu.VMEM((3, ring, capacity) + block, jnp.bfloat16),
            pltpu.VMEM((3, ring * capacity, LANES), jnp.float32),
            pltpu.VMEM((2, ring, half) + block, jnp.bfloat16),
            pltpu.VMEM((2, steps, tiles) + block, jnp.bfloat16),
            pltpu.VMEM((2, steps, tiles) + block, jnp.bfloat16),
            pltpu.VMEM((4 * capacity, LANES), jnp.float32),
            pltpu.VMEM((ring, tiles, 4 * capacity, LANES), jnp.float32),
            pltpu.VMEM((CHUNK,) + block, jnp.float32),
            pltpu.VMEM((ring, tiles) + answer, jnp.bfloat16),
            pltpu.VMEM((3, ring, capacity) + answer, jnp.bfloat16),
            pltpu.VMEM((2, ring, half) + answer, jnp.bfloat16),
            pltpu.VMEM((2, 2 * EDGE, width), jnp.float32),
            pltpu.VMEM((2, PLANE, 3 * width), jnp.bfloat16),
            pltpu.VMEM((2, 4 * EDGE, 3 * width), jnp.bfloat16),
            pltpu.VMEM((blocks, 3, width), jnp.float32),
            pltpu.VMEM((blocks, 9, width), jnp.float32),
            dma((6,)),
            dma((3,)),
            dma((3,)),
            dma((ring, 6)),
            dma((ring, 6)),
            dma((2, steps, chunks)),
            dma((2, steps, chunks)),
            dma((2, steps, chunks)),
            dma((2, steps, chunks)),
            dma((ring, 6)),
            dma((ring, 6)),
        ]
        + [pltpu.VMEM((side * capacity,) + answer, jnp.bfloat16)] * ring,
        compiler_params=pltpu.CompilerParams(
            collective_id=0, has_side_effects=True, vmem_limit_bytes=62 << 20
        ),
        cost_estimate=pl.CostEstimate(flops=1 << 32, bytes_accessed=8 << 20, transcendentals=0),
        name="transfer",
    )(
        *lists,
        names.reshape(side, ring * capacity, LANES),
        stages,
        mass.reshape(1, -1),
        motion,
        affine,
        cell,
        fraction,
        drag,
    )


def per_device(
    particle_mass,
    particle_velocity,
    particle_affine,
    particle_cell,
    particle_fraction,
    block_owner,
    block_slot,
    block_count,
    cell_drag,
):
    ring, side = lax.axis_size("gy"), lax.axis_size("gz")
    blocks = block_count.shape[0]
    capacity = max(1, 2 * blocks // (ring * side))
    tiles = cell_drag.shape[0]
    plan = make_plan(block_owner.reshape(-1), block_slot, block_count, ring, side, capacity)
    velocity, new_velocity, new_affine = transfer(
        plan,
        blocks,
        particle_mass,
        particle_velocity,
        particle_affine,
        particle_cell,
        particle_fraction,
        cell_drag.reshape(tiles, EDGE, PLANE),
        ring,
        side,
        capacity,
    )
    return (velocity.reshape(tiles, 3, -1), new_velocity, new_affine)


def solution(mesh):
    split = ("gx", "gy", "gz")
    return jax.shard_map(
        per_device,
        mesh=mesh,
        in_specs=(
            P(split),
            P(None, split),
            P(None, split),
            P(None, split),
            P(None, split),
            P(split, None),
            P(split),
            P(split),
            P(split, None),
        ),
        out_specs=(P(split, None, None), P(None, split), P(None, split)),
        check_vma=False,
    )
```
